32 devices in a mesh: dp: 4 (over y, x), row: 2 (over core), col: 4 (over z).
Axes of the slice: x: 2, y: 2, z: 4, core: 2. Of those that a mesh axis runs over, the one named last changes fastest.
Arguments:
- tokens: bfloat16 [3840, 4096], P(('dp', 'col'), 'row'), may hold values from -6 to 6
- hidden_cot: bfloat16 [3840, 14336], P(('dp', 'row'), 'col'), may hold values from -0.09667969 to 0.09667969
- gate_pre: bfloat16 [3840, 14336], P(('dp', 'row'), 'col'), may hold values from -10 to 10
- up_pre: bfloat16 [3840, 14336], P(('dp', 'row'), 'col'), may hold values from -6 to 6
Outputs:
- grad_gate: bfloat16 [2, 2048, 14336], P('row', 'dp', 'col')
The draws below stay inside these ranges and needn't reach their ends.
All inputs are finite; a program needn't handle non-finite values.
Results may differ from the reference program's by a relative error of at most 0.014.
Values may be sent and summed in bfloat16 or wider, within the bound.
A program may use at most 128 MiB of HBM per device.

```python
import jax
import jax.numpy as jnp
from jax import lax

D = 4096
FF = 14336
GROUP_TOK = 960
TOKENS = 3840
N_DP = 4
N_ROW = 2


def level_of(own_key, shape, split, least, high):
    def one(dim, parts):
        heights = jax.random.uniform(jax.random.fold_in(jax.random.fold_in(own_key, 6), dim), (parts,), jnp.float32, least / len(split), high / len(split))
        return jnp.repeat(jnp.exp(heights), shape[dim] // parts).reshape((-1,) + (1,) * (len(shape) - dim - 1))

    gain = one(*split[0])
    for cut in split[1:]:
        gain = gain * one(*cut)
    return gain


def scatter_about(own_key, dims, deviation, most, shards=(), held_as=jnp.bfloat16):
    drawn = deviation * jax.random.normal(own_key, dims, jnp.float32)
    if shards:
        drawn = drawn * level_of(own_key, dims, shards, -0.22, 0.18)
    return jnp.clip(drawn, -most, most).astype(held_as)


def setup_inputs(seed: int = 0) -> dict:
    seeds = jax.random.split(jax.random.key(seed), 5)
    return {
        "tokens": scatter_about(seeds[0], (TOKENS, D), 1.0, 6.0, ((0, 16), (1, 2))),
        "hidden_cot": scatter_about(seeds[1], (TOKENS, FF), (TOKENS ** -0.5), 0.09667969, ((0, 8), (1, 4))),
        "gate_pre": scatter_about(seeds[2], (TOKENS, FF), 2.0, 10.0, ((0, 8), (1, 4))),
        "up_pre": scatter_about(seeds[3], (TOKENS, FF), 1.0, 6.0, ((0, 8), (1, 4))),
    }


def reference(tokens, hidden_cot, gate_pre, up_pre):
    gate_val = gate_pre.astype(jnp.float32)
    up_val = up_pre.astype(jnp.float32)
    cot_val = hidden_cot.astype(jnp.float32)
    sigma = jax.nn.sigmoid(gate_val)
    gate_grad = (cot_val * up_val * sigma * (1.0 + gate_val * (1.0 - sigma))).astype(jnp.bfloat16)
    tok_groups = tokens.reshape(N_DP, GROUP_TOK, D)
    grad_groups = gate_grad.reshape(N_DP, GROUP_TOK, FF)

    def one_group(total, pair):
        part = jnp.dot(pair[0].T, pair[1], preferred_element_type=jnp.float32).astype(jnp.bfloat16)
        return total + part.astype(jnp.float32), None

    summed, _ = lax.scan(one_group, jnp.zeros((D, FF), jnp.float32), (tok_groups, grad_groups))
    return summed.astype(jnp.bfloat16).reshape(N_ROW, D // N_ROW, FF)
```

```python
import functools
import math

import jax
import jax.numpy as jnp
from jax import lax
from jax.experimental import pallas as pl
from jax.experimental.pallas import tpu as pltpu
from jax.sharding import PartitionSpec as P

MESH = pl.DeviceIdType.MESH


def near_square(n):
    nx = math.isqrt(n)
    while n % nx:
        nx -= 1
    return n // nx, nx


def kernel(dims, starts, tok, cot, gate, up, out, ins, grads, toks, tokt, part, got, res,
           in_sem, own_sem, ty_s, ty_r, tz_s, tz_r, gy_s, gy_r, gp_s, gp_r, x_s, x_r, out_sem):
    ny, nx, nr, nz, wide, block, chunks, cols = dims
    dp, r, z = lax.axis_index("dp"), lax.axis_index("row"), lax.axis_index("col")
    y, x = dp // nx, dp % nx
    subs = wide // block
    away = (nx - 1) * subs
    blocks = nx * subs
    rows = ny * nr * grads.shape[3]

    def at(oy=0, ox=0, orow=0, oz=0):
        return {
            "dp": (y + oy) % ny * nx + (x + ox) % nx,
            "row": (r + orow) % nr,
            "col": (z + oz) % nz,
        }

    def remote(src, dst, ss, rs, to):
        return pltpu.make_async_remote_copy(
            src_ref=src, dst_ref=dst, send_sem=ss, recv_sem=rs, device_id=to, device_id_type=MESH)

    def each(n, f):
        def body(i, c):
            f(i)
            return c
        lax.fori_loop(0, n, body, 0)

    def load(k, i):
        src = (cot, gate, up)[i]
        return pltpu.make_async_copy(
            src.at[:, pl.ds(pl.multiple_of(k * cols, cols), cols)], ins.at[i, k], in_sem.at[i, k])

    def tok_cols(oy, b):
        o, sub = (b // subs + 1) % nx, b % subs
        first = ((y + oy) % ny * nx + (x + o) % nx) * wide + sub * block
        return tok.at[:, pl.ds(pl.multiple_of(first, block), block)]

    def own_tok(b):
        return pltpu.make_async_copy(tok_cols(0, b), toks.at[b, y, z], own_sem.at[b])

    def tok_y(oy, b):
        return remote(tok_cols(oy, b), toks.at[b, y, z], ty_s.at[oy - 1, b], ty_r.at[oy - 1, b], at(oy=oy))

    def tok_z(oz, b, oy):
        ref = toks.at[b, (y - oy + ny) % ny, z]
        return remote(ref, ref, tz_s.at[oz - 1, b, oy], tz_r.at[oz - 1, b, oy], at(oz=oz))

    def grad_y(oy, k):
        ref = grads.at[k, y, r]
        return remote(ref, ref, gy_s.at[oy - 1, k], gy_r.at[oy - 1, k], at(oy=oy))

    def grad_p(orow, oy, k):
        ref = grads.at[k, (y - oy + ny) % ny, r]
        return remote(ref, ref, gp_s.at[orow - 1, oy, k], gp_r.at[orow - 1, oy, k], at(orow=orow))

    def sum_x(b, k):
        return remote(part.at[b, k], got.at[b, k], x_s.at[b, k], x_r.at[b, k], at(ox=b // subs + 1))

    def write(sub, k):
        return pltpu.make_async_copy(
            res.at[sub, k],
            out.at[0, pl.ds(sub * block, block), pl.ds(pl.multiple_of(k * cols, cols), cols)],
            out_sem.at[sub, k])

    for b in range(blocks):
        own_tok(b).start()

    def load_all(k):
        for i in range(3):
            load(k, i).start()
    each(chunks, load_all)

    peers = ([at(oy=o) for o in range(1, ny)] + [at(ox=o) for o in range(1, nx)]
             + [at(orow=o) for o in range(1, nr)] + [at(oz=o) for o in range(1, nz)])
    barrier = pltpu.get_barrier_semaphore()
    for to in peers:
        pl.semaphore_signal(barrier, inc=1, device_id=to, device_id_type=MESH)
    pl.semaphore_wait(barrier, len(peers))

    for b in range(blocks):
        for oy in range(1, ny):
            tok_y(oy, b).start()

    def own_out(b):
        own_tok(b).wait()
        for oz in range(1, nz):
            tok_z(oz, b, 0).start()

    def pass_on(b):
        for oy in range(1, ny):
            tok_y(oy, b).wait_recv()
            for oz in range(1, nz):
                tok_z(oz, b, oy).start()

    def gate_grad(k):
        for i in range(3):
            load(k, i).wait()
        step = 32
        tall = ins.shape[2]

        def rows_of(j, c):
            at_rows = pl.ds(pl.multiple_of(j * step, step), step)
            h = ins[0, k, at_rows, :].astype(jnp.float32)
            g = ins[1, k, at_rows, :].astype(jnp.float32)
            u = ins[2, k, at_rows, :].astype(jnp.float32)
            s = jax.nn.sigmoid(g)
            grads[k, y, r, at_rows, :] = (h * u * s * (1.0 + g * (1.0 - s))).astype(grads.dtype)
            return c
        lax.fori_loop(0, tall // step, rows_of, 0)
        for oy in range(1, ny):
            grad_y(oy, k).start()
        for orow in range(1, nr):
            grad_p(orow, 0, k).start()

    for b in range(away):
        own_out(b)
    early = min(4, chunks)
    each(early, gate_grad)
    for b in range(away):
        pass_on(b)
    for b in range(away, blocks):
        own_out(b)
    each(chunks - early, lambda k: gate_grad(k + early))
    for b in range(away, blocks):
        pass_on(b)

    def arrive(k):
        for oy in range(1, ny):
            grad_y(oy, k).wait_recv()
            for orow in range(1, nr):
                grad_p(orow, oy, k).start()
        for orow in range(1, nr):
            for oy in range(ny):
                grad_p(orow, oy, k).wait_recv()

    def take_block(b):
        for oz in range(1, nz):
            for oy in range(ny):
                tok_z(oz, b, oy).wait_recv()
        tokt[b] = toks[b].reshape(rows, block).T

    def product(b, k):
        return jnp.dot(tokt[b], grads[k].reshape(rows, cols), preferred_element_type=jnp.float32)

    def tile(b, k):
        part[b, k] = product(b, k).astype(part.dtype)
        sum_x(b, k).start()

    begins = [min(starts[min(b, len(starts) - 1)], chunks - 1) for b in range(away)]
    live, done = [], 0
    for now in sorted(set(begins)) + [chunks]:
        def stretch(i, live=tuple(live), done=done):
            arrive(i + done)
            for b in live:
                tile(b, i + done)
        if now > done:
            each(now - done, stretch)
        done = now
        for b in range(away):
            if now < chunks and begins[b] == now:
                take_block(b)
                if now:
                    each(now, functools.partial(tile, b))
                live.append(b)

    for b in range(away, blocks):
        take_block(b)

    def finish(k):
        for sub in range(subs):
            total = product(away + sub, k)
            for o in range(1, nx):
                b = (o - 1) * subs + sub
                sum_x(b, k).wait_recv()
                total = total + got[b, k].astype(jnp.float32)
            res[sub, k] = total.astype(res.dtype)
            write(sub, k).start()
    each(chunks, finish)

    for b in range(blocks):
        for oy in range(1, ny):
            tok_y(oy, b).wait_send()
        for oz in range(1, nz):
            for oy in range(ny):
                tok_z(oz, b, oy).wait_send()

    def drain(k):
        for oy in range(1, ny):
            grad_y(oy, k).wait_send()
        for orow in range(1, nr):
            for oy in range(ny):
                grad_p(orow, oy, k).wait_send()
        for b in range(away):
            sum_x(b, k).wait_send()
        for sub in range(subs):
            write(sub, k).wait()
    each(chunks, drain)


def solution(mesh):
    ndp, nr, nz = mesh.shape["dp"], mesh.shape["row"], mesh.shape["col"]
    ny, nx = near_square(ndp)

    def on_device(tokens, hidden_cot, gate_pre, up_pre):
        tok_rows, wid = tokens.shape
        tall, hidden = gate_pre.shape
        wide = wid // ndp
        block = math.gcd(wide, 256)
        cols = math.gcd(hidden, 256)
        chunks = hidden // cols
        subs = wide // block
        blocks, away = nx * subs, (nx - 1) * subs
        rows = ny * nz * tok_rows
        dims = (ny, nx, nr, nz, wide, block, chunks, cols)
        starts = (2, 6)
        dma = pltpu.SemaphoreType.DMA
        dt = tokens.dtype
        return pl.pallas_call(
            functools.partial(kernel, dims, starts),
            out_shape=jax.ShapeDtypeStruct((1, wide, hidden), dt),
            in_specs=[pl.BlockSpec(memory_space=pl.ANY)] * 4,
            out_specs=pl.BlockSpec(memory_space=pl.ANY),
            scratch_shapes=[
                pltpu.VMEM((3, chunks, tall, cols), dt),
                pltpu.VMEM((chunks, ny, nr, tall, cols), dt),
                pltpu.VMEM((blocks, ny, nz, tok_rows, block), dt),
                pltpu.VMEM((blocks, block, rows), dt),
                pltpu.VMEM((max(away, 1), chunks, block, cols), dt),
                pltpu.VMEM((max(away, 1), chunks, block, cols), dt),
                pltpu.VMEM((subs, chunks, block, cols), dt),
                dma((3, chunks)),
                dma((blocks,)),
                dma((max(ny - 1, 1), blocks)),
                dma((max(ny - 1, 1), blocks)),
                dma((max(nz - 1, 1), blocks, ny)),
                dma((max(nz - 1, 1), blocks, ny)),
                dma((max(ny - 1, 1), chunks)),
                dma((max(ny - 1, 1), chunks)),
                dma((max(nr - 1, 1), ny, chunks)),
                dma((max(nr - 1, 1), ny, chunks)),
                dma((max(away, 1), chunks)),
                dma((max(away, 1), chunks)),
                dma((subs, chunks)),
            ],
            compiler_params=pltpu.CompilerParams(
                collective_id=0, has_side_effects=True, vmem_limit_bytes=63 * 1024 * 1024
            ),
        )(tokens, hidden_cot, gate_pre, up_pre)

    in_specs = (
        P(("dp", "col"), "row"),
        P(("dp", "row"), "col"),
        P(("dp", "row"), "col"),
        P(("dp", "row"), "col"),
    )
    return jax.shard_map(
        on_device, mesh=mesh, in_specs=in_specs, out_specs=P("row", "dp", "col"), check_vma=False
    )
```

```python
import functools
import math

import jax
import jax.numpy as jnp
from jax import lax
from jax.experimental import pallas as pl
from jax.experimental.pallas import tpu as pltpu
from jax.sharding import PartitionSpec as P

MESH = pl.DeviceIdType.MESH


def near_square(n):
    nx = math.isqrt(n)
    while n % nx:
        nx -= 1
    return n // nx, nx


def kernel(dims, plan, tok, cot, gate, up, out, ins, grads, toks, tokt, part, got, res,
           in_sem, own_sem, ty_s, ty_r, tz_s, tz_r, gy_s, gy_r, gp_s, gp_r, x_s, x_r, out_sem):
    ny, nx, nr, nz, wide, block, chunks, cols = dims
    ahead, own_at = plan
    dp, r, z = lax.axis_index("dp"), lax.axis_index("row"), lax.axis_index("col")
    y, x = dp // nx, dp % nx
    subs = wide // block
    away = (nx - 1) * subs
    blocks = nx * subs
    rows = ny * nr * grads.shape[3]

    def at(oy=0, ox=0, orow=0, oz=0):
        return {
            "dp": (y + oy) % ny * nx + (x + ox) % nx,
            "row": (r + orow) % nr,
            "col": (z + oz) % nz,
        }

    def remote(src, dst, ss, rs, to):
        return pltpu.make_async_remote_copy(
            src_ref=src, dst_ref=dst, send_sem=ss, recv_sem=rs, device_id=to, device_id_type=MESH)

    def each(n, f):
        def body(i, c):
            f(i)
            return c
        lax.fori_loop(0, n, body, 0)

    def load(k, i):
        src = (cot, gate, up)[i]
        return pltpu.make_async_copy(
            src.at[:, pl.ds(pl.multiple_of(k * cols, cols), cols)], ins.at[i, k], in_sem.at[i, k])

    def tok_cols(oy, b):
        o, sub = (b // subs + 1) % nx, b % subs
        first = ((y + oy) % ny * nx + (x + o) % nx) * wide + sub * block
        return tok.at[:, pl.ds(pl.multiple_of(first, block), block)]

    def own_tok(b):
        return pltpu.make_async_copy(tok_cols(0, b), toks.at[b, y, z], own_sem.at[b])

    def tok_y(oy, b):
        return remote(tok_cols(oy, b), toks.at[b, y, z], ty_s.at[oy - 1, b], ty_r.at[oy - 1, b], at(oy=oy))

    reach = min(2, nz - 1)
    hops = ([(d, 0) for d in range(1, reach + 1)] + [(1, d) for d in range(2, nz - 1)])

    def valid(way, far, back):
        left = z >= back if way > 0 else z + back < nz
        right = z + far < nz if way > 0 else z >= far
        return jnp.logical_and(left, right)

    def tok_z(b, oy, way, i):
        far, back = hops[i]
        zs = z - way * back
        ref = toks.at[b, (y - oy + ny) % ny, zs]
        w = 0 if way > 0 else 1
        return remote(ref, ref, tz_s.at[w, i, b, oy], tz_r.at[zs, b, oy], at(oz=way * far + nz))

    def send_z(b, oy, relay, act):
        for way in (1, -1):
            for i, (far, back) in enumerate(hops):
                if (back > 0) == relay:
                    pl.when(valid(way, far, back))(functools.partial(lambda w, n: act(tok_z(b, oy, w, n)), way, i))

    def got_z(b, oy, zs):
        ref = toks.at[b, (y - oy + ny) % ny, zs]
        return remote(ref, ref, tz_s.at[0, 0, b, oy], tz_r.at[zs, b, oy], at(oz=1))

    def relay_z(b):
        for oy in range(ny):
            for way in (1, -1):
                for i, (far, back) in enumerate(hops):
                    if back:
                        def go(way=way, i=i, back=back, oy=oy):
                            got_z(b, oy, z - way * back).wait_recv()
                            tok_z(b, oy, way, i).start()
                        pl.when(valid(way, far, back))(go)

    def all_z(b):
        for oy in range(ny):
            for zs in range(nz):
                seen = jnp.bool_(False)
                for way in (1, -1):
                    for far, back in hops:
                        if back:
                            seen = jnp.logical_or(seen, jnp.logical_and(valid(way, far, back), z - way * back == zs))
                pl.when(jnp.logical_and(z != zs, jnp.logical_not(seen)))(got_z(b, oy, zs).wait_recv)

    def grad_y(oy, k):
        ref = grads.at[k, y, r]
        return remote(ref, ref, gy_s.at[oy - 1, k], gy_r.at[oy - 1, k], at(oy=oy))

    def grad_p(orow, oy, k):
        ref = grads.at[k, (y - oy + ny) % ny, r]
        return remote(ref, ref, gp_s.at[orow - 1, oy, k], gp_r.at[orow - 1, oy, k], at(orow=orow))

    def sum_x(b, k):
        return remote(part.at[b, k], got.at[b, k], x_s.at[b, k], x_r.at[b, k], at(ox=b // subs + 1))

    def write(sub, k):
        return pltpu.make_async_copy(
            res.at[sub, k],
            out.at[0, pl.ds(sub * block, block), pl.ds(pl.multiple_of(k * cols, cols), cols)],
            out_sem.at[sub, k])

    for b in range(blocks):
        own_tok(b).start()

    def load_all(k):
        for i in range(3):
            load(k, i).start()
    each(chunks, load_all)

    peers = ([at(oy=o) for o in range(1, ny)] + [at(ox=o) for o in range(1, nx)]
             + [at(orow=o) for o in range(1, nr)] + [at(oz=o) for o in range(1, nz)])
    barrier = pltpu.get_barrier_semaphore()
    for to in peers:
        pl.semaphore_signal(barrier, inc=1, device_id=to, device_id_type=MESH)
    pl.semaphore_wait(barrier, len(peers))

    def tok_out(b):
        for oy in range(1, ny):
            tok_y(oy, b).start()

    def own_out(b):
        own_tok(b).wait()
        send_z(b, 0, False, lambda c: c.start())

    def pass_on(b):
        for oy in range(1, ny):
            tok_y(oy, b).wait_recv()
            send_z(b, oy, False, lambda c: c.start())

    def gate_grad(k):
        for i in range(3):
            load(k, i).wait()
        step = 32
        tall = ins.shape[2]

        def rows_of(j, c):
            at_rows = pl.ds(pl.multiple_of(j * step, step), step)
            h = ins[0, k, at_rows, :].astype(jnp.float32)
            g = ins[1, k, at_rows, :].astype(jnp.float32)
            u = ins[2, k, at_rows, :].astype(jnp.float32)
            s = jax.nn.sigmoid(g)
            grads[k, y, r, at_rows, :] = (h * u * s * (1.0 + g * (1.0 - s))).astype(grads.dtype)
            return c
        lax.fori_loop(0, tall // step, rows_of, 0)
        for oy in range(1, ny):
            grad_y(oy, k).start()
        for orow in range(1, nr):
            grad_p(orow, 0, k).start()

    def feed(k):
        gate_grad(k)
        pl.when(k + lead < blocks)(lambda: tok_out(k + lead))

    def take_block(b):
        all_z(b)
        first = pl.multiple_of(b * block, block)
        tokt[pl.ds(first, block), :] = toks[b].reshape(rows, block).T

    def tile(b, k):
        left = tokt[pl.ds(pl.multiple_of(b * block, block), block), :]
        right = grads[k].reshape(rows, cols)
        part[b, k] = jnp.dot(left, right, preferred_element_type=jnp.float32).astype(part.dtype)
        sum_x(b, k).start()

    def finish(k):
        left = tokt[away * block:, :]
        total = jnp.dot(left, grads[k].reshape(rows, cols), preferred_element_type=jnp.float32)
        for sub in range(subs):
            sums = total[sub * block:(sub + 1) * block]
            for o in range(1, nx):
                b = (o - 1) * subs + sub
                sum_x(b, k).wait_recv()
                sums = sums + got[b, k].astype(jnp.float32)
            res[sub, k] = sums.astype(res.dtype)
            write(sub, k).start()

    def span(low, high, f):
        def body(i, c):
            f(i)
            return c
        lax.fori_loop(low, high, body, 0)

    def z_out(b):
        own_out(b)
        pass_on(b)

    def z_step(j):
        relay_z(j)
        pl.when(j + lead < blocks)(lambda: z_out(j + lead))

    relayed = lambda k: jnp.where(k >= own_at, blocks, jnp.minimum((2 * k + 5) * blocks // 24, blocks))
    ready = lambda k: jnp.where(k >= own_at, away, jnp.minimum((2 * k + 3) * away // 12, away))
    ended = lambda k: jnp.clip((k - own_at + 1) * 3, 0, chunks - 3)

    lead = min(2, blocks)
    for b in range(lead):
        tok_out(b)
    for b in range(lead):
        own_out(b)
    for b in range(lead):
        feed(b)
        pass_on(b)
    span(lead, ahead, feed)

    def main(k, c):
        pl.when(k + ahead < chunks)(lambda: feed(k + ahead))
        span(jnp.where(k > 0, relayed(k - 1), 0), relayed(k), z_step)
        for oy in range(1, ny):
            grad_y(oy, k).wait_recv()
            for orow in range(1, nr):
                grad_p(orow, oy, k).start()

        def catch_up(b):
            take_block(b)
            span(0, k, functools.partial(tile, b))
        now = ready(k)
        span(jnp.where(k > 0, ready(k - 1), 0), now, catch_up)

        @pl.when(k == own_at)
        def _():
            span(away, blocks, take_block)
        span(ended(k - 1), ended(k), finish)
        for orow in range(1, nr):
            for oy in range(ny):
                grad_p(orow, oy, k).wait_recv()
        span(0, now, lambda b: tile(b, k))
        return c
    lax.fori_loop(0, chunks, main, 0)
    span(ended(chunks - 1), chunks, finish)

    def done(b):
        for oy in range(1, ny):
            tok_y(oy, b).wait_send()
        for oy in range(ny):
            for relay in (False, True):
                send_z(b, oy, relay, lambda c: c.wait_send())
    each(blocks, done)

    def drain(k):
        for oy in range(1, ny):
            grad_y(oy, k).wait_send()
        for orow in range(1, nr):
            for oy in range(ny):
                grad_p(orow, oy, k).wait_send()
        for b in range(away):
            sum_x(b, k).wait_send()
        for sub in range(subs):
            write(sub, k).wait()
    each(chunks, drain)


def solution(mesh):
    ndp, nr, nz = mesh.shape["dp"], mesh.shape["row"], mesh.shape["col"]
    ny, nx = near_square(ndp)

    def on_device(tokens, hidden_cot, gate_pre, up_pre):
        tok_rows, wid = tokens.shape
        tall, hidden = gate_pre.shape
        wide = wid // ndp
        block = math.gcd(wide, 128)
        cols = math.gcd(hidden, 256)
        chunks = hidden // cols
        subs = wide // block
        blocks, away = nx * subs, (nx - 1) * subs
        rows = ny * nz * tok_rows
        dims = (ny, nx, nr, nz, wide, block, chunks, cols)
        plan = (min(8, chunks), max(chunks - 5, 0))
        dma = pltpu.SemaphoreType.DMA
        dt = tokens.dtype
        return pl.pallas_call(
            functools.partial(kernel, dims, plan),
            out_shape=jax.ShapeDtypeStruct((1, wide, hidden), dt),
            in_specs=[pl.BlockSpec(memory_space=pl.ANY)] * 4,
            out_specs=pl.BlockSpec(memory_space=pl.ANY),
            scratch_shapes=[
                pltpu.VMEM((3, chunks, tall, cols), dt),
                pltpu.VMEM((chunks, ny, nr, tall, cols), dt),
                pltpu.VMEM((blocks, ny, nz, tok_rows, block), dt),
                pltpu.VMEM((blocks * block, rows), dt),
                pltpu.VMEM((max(away, 1), chunks, block, cols), dt),
                pltpu.VMEM((max(away, 1), chunks, block, cols), dt),
                pltpu.VMEM((subs, chunks, block, cols), dt),
                dma((3, chunks)),
                dma((blocks,)),
                dma((max(ny - 1, 1), blocks)),
                dma((max(ny - 1, 1), blocks)),
                dma((2, max(2 * nz, 1), blocks, ny)),
                dma((nz, blocks, ny)),
                dma((max(ny - 1, 1), chunks)),
                dma((max(ny - 1, 1), chunks)),
                dma((max(nr - 1, 1), ny, chunks)),
                dma((max(nr - 1, 1), ny, chunks)),
                dma((max(away, 1), chunks)),
                dma((max(away, 1), chunks)),
                dma((subs, chunks)),
            ],
            compiler_params=pltpu.CompilerParams(
                collective_id=0, has_side_effects=True, vmem_limit_bytes=63 * 1024 * 1024
            ),
        )(tokens, hidden_cot, gate_pre, up_pre)

    in_specs = (
        P(("dp", "col"), "row"),
        P(("dp", "row"), "col"),
        P(("dp", "row"), "col"),
        P(("dp", "row"), "col"),
    )
    return jax.shard_map(
        on_device, mesh=mesh, in_specs=in_specs, out_specs=P("row", "dp", "col"), check_vma=False
    )
```
